32 devices in a mesh: gx: 8 (over y, x, core), gy: 4 (over z).
Axes of the slice: x: 2, y: 2, z: 4, core: 2. Of those that a mesh axis runs over, the one named last changes fastest.
Arguments:
- nodes: bfloat16 [32768, 128], P(('gx', 'gy')), may hold values from -6 to 6
- ghost_rows: int32 [32, 8, 256], P(('gx', 'gy')), may hold values from 0 to 1023
- ghost_count: int32 [32, 8], P(('gx', 'gy')), may hold values from 0 to 256, as said below
- edge_send: int32 [32, 4096], P(('gx', 'gy')), may hold values from 0 to 3071
- edge_recv: int32 [32, 4096], P(('gx', 'gy')), may hold values from 0 to 1023
- edge_count: int32 [32], P(('gx', 'gy')), may hold values from 512 to 4096, as said below
- pool_map: int32 [32, 1024], P(('gx', 'gy')), may hold values from 0 to 191, as said below
- w_edge_in: bfloat16 [256, 128], replicated, may hold values from -0.375 to 0.375
- w_edge_out: bfloat16 [128, 128], replicated, may hold values from -0.5 to 0.5
- w_node_in: bfloat16 [256, 128], replicated, may hold values from -0.375 to 0.375
- w_node_out: bfloat16 [128, 128], replicated, may hold values from -0.5 to 0.5
- w_coarse_in: bfloat16 [128, 128], replicated, may hold values from -0.5 to 0.5
- w_coarse_out: bfloat16 [128, 128], replicated, may hold values from -0.5 to 0.5
- d_fine: bfloat16 [32768, 128], P(('gx', 'gy')), may hold values from -6 to 6
- d_coarse: bfloat16 [4096, 128], P(('gx', 'gy')), may hold values from -6 to 6
Outputs:
- fine_out: bfloat16 [32768, 128], P(('gx', 'gy'))
- coarse_out: bfloat16 [4096, 128], P(('gx', 'gy'))
- grad_nodes: float32 [32768, 128], P(('gx', 'gy'))
- grad_edge_in: float32 [256, 128], replicated
- grad_edge_out: float32 [128, 128], replicated
- grad_node_in: float32 [256, 128], replicated
- grad_node_out: float32 [128, 128], replicated
- grad_coarse_in: float32 [128, 128], replicated
- grad_coarse_out: float32 [128, 128], replicated
The draws below stay inside these ranges and needn't reach their ends.
Inputs may be any that keep to these rules, and one draw needn't show every extreme that they name: `ghost_count`: every device fills all 256 slots for at least one offset. `edge_count`: at least one device has all 4096 slots live. `pool_map`: values under 32 occur only on devices that are not first along gy, and values of 160 or more only on devices that are not last along gy, so every parent lies in the device's gx column.
All inputs are finite; a program needn't handle non-finite values.
Results may differ from the reference program's by a relative error of at most 0.012.
Values may be sent and summed in bfloat16 or wider, within the bound.
A program may use at most 64 MiB of HBM per device.

```python
import jax
import jax.numpy as jnp
from jax import lax

C = 128
HID = 128
GBLK = 256
BAND = 32
NODE_DEV = 1024
EDGE_DEV = 4096
CO_DEV = 128
NODES = 32768
COARSE = 4096
N_GX = 8
N_GY = 4
DEVICES = 32


def draw_ghost_count(key, part):
    key_one, key_two = jax.random.split(jax.random.fold_in(key, 11))
    counts = jax.random.randint(key_one, (N_GX * N_GY, 8), 0, GBLK + 1)
    full_peer = jax.random.randint(key_two, (N_GX * N_GY, 1), 0, 8)
    direction_ids = jnp.arange(8, dtype=jnp.int32)[None, :]
    return jnp.where(direction_ids == full_peer, GBLK, counts).astype(jnp.int32)


def draw_edge_count(key, part):
    key_one, key_two = jax.random.split(jax.random.fold_in(key, 23))
    shifts = jax.random.randint(key_one, (N_GX * N_GY,), 0, 4).astype(jnp.int32)
    counts = jnp.right_shift(jnp.full((N_GX * N_GY,), EDGE_DEV, jnp.int32), shifts)
    busiest = jax.random.randint(key_two, (), 0, N_GX * N_GY)
    device_ids = jnp.arange(N_GX * N_GY, dtype=jnp.int32)
    return jnp.where(device_ids == busiest, EDGE_DEV, counts).astype(jnp.int32)


def draw_pool_map(key, part):
    devices = N_GX * N_GY
    near = max(1, NODE_DEV // 16)
    key_one, key_two, key_three, key_four = jax.random.split(jax.random.fold_in(key, 37), 4)
    order = jax.vmap(lambda single: jax.random.permutation(single, NODE_DEV))(jax.random.split(key_one, devices))
    own_parent = jax.random.randint(key_two, (devices, NODE_DEV), BAND, BAND + CO_DEV)
    lower_parent = jax.random.randint(key_three, (devices, NODE_DEV), 0, BAND)
    upper_parent = jax.random.randint(key_four, (devices, NODE_DEV), BAND + CO_DEV, CO_DEV + 2 * BAND)
    row_idx = (jnp.arange(devices, dtype=jnp.int32) % N_GY)[:, None]
    goes_lower = (order < near) & (row_idx > 0)
    goes_upper = (order >= near) & (order < 2 * near) & (row_idx < N_GY - 1)
    return jnp.where(goes_lower, lower_parent, jnp.where(goes_upper, upper_parent, own_parent)).astype(jnp.int32)


def set_ends(drawn, own_key, low, top_value):
    longest = drawn.shape.index(max(drawn.shape))
    spots = []
    for shift in (0, 1):
        where = [jax.random.randint(jax.random.fold_in(own_key, axis), (), 0, length) for axis, length in enumerate(drawn.shape)]
        where[longest] = (where[longest] + shift) % drawn.shape[longest]
        spots.append(tuple(where))
    return drawn.at[spots[0]].set(low).at[spots[1]].set(top_value)


def level_of(key, dims, cuts, smallest, largest):
    def one(axis_at, blocks):
        draws = jax.random.uniform(jax.random.fold_in(jax.random.fold_in(key, 6), axis_at), (blocks,), jnp.float32, smallest / len(cuts), largest / len(cuts))
        return jnp.repeat(jnp.exp(draws), dims[axis_at] // blocks).reshape((-1,) + (1,) * (len(dims) - axis_at - 1))

    loudness = one(*cuts[0])
    for cut in cuts[1:]:
        loudness = loudness * one(*cut)
    return loudness


def normal_values(rng, dims, scale, reach, shards=(), kind=jnp.bfloat16):
    gain = level_of(rng, dims, shards, -0.22, 0.18) if shards else 1.0
    entries = jax.random.normal(rng, dims, jnp.float32) * scale * gain
    return jnp.minimum(jnp.maximum(entries, -reach), reach).astype(kind)


def setup_inputs(seed: int = 0) -> dict:
    splits = jax.random.split(jax.random.key(seed), 16)
    return {
        "nodes": normal_values(splits[0], (NODES, C), 1.0, 6.0, ((0, 32),)),
        "ghost_rows": set_ends(jax.random.randint(splits[1], (DEVICES, 8, GBLK), 0, NODE_DEV), jax.random.fold_in(splits[1], 1), 0, NODE_DEV - 1).astype(jnp.int32),
        "ghost_count": draw_ghost_count(jax.random.fold_in(splits[15], 71), 0),
        "edge_send": set_ends(jax.random.randint(splits[3], (DEVICES, EDGE_DEV), 0, NODE_DEV + 8 * GBLK), jax.random.fold_in(splits[3], 1), 0, (NODE_DEV + 8 * GBLK) - 1).astype(jnp.int32),
        "edge_recv": set_ends(jax.random.randint(splits[4], (DEVICES, EDGE_DEV), 0, NODE_DEV), jax.random.fold_in(splits[4], 1), 0, NODE_DEV - 1).astype(jnp.int32),
        "edge_count": draw_edge_count(jax.random.fold_in(splits[15], 71), 0),
        "pool_map": draw_pool_map(jax.random.fold_in(splits[15], 71), 0),
        "w_edge_in": normal_values(splits[7], (2 * C, HID), (2 * C) ** -0.5, 0.375),
        "w_edge_out": normal_values(splits[8], (HID, C), HID ** -0.5, 0.5),
        "w_node_in": normal_values(splits[9], (2 * C, HID), (2 * C) ** -0.5, 0.375),
        "w_node_out": normal_values(splits[10], (HID, C), HID ** -0.5, 0.5),
        "w_coarse_in": normal_values(splits[11], (C, HID), C ** -0.5, 0.5),
        "w_coarse_out": normal_values(splits[12], (HID, C), HID ** -0.5, 0.5),
        "d_fine": normal_values(splits[13], (NODES, C), 1.0, 6.0, ((0, 32),)),
        "d_coarse": normal_values(splits[14], (COARSE, C), 1.0, 6.0, ((0, 32),)),
    }


offset_across = (-1, -1, -1, 0, 0, 1, 1, 1)
offset_along = (-1, 0, 1, -1, 1, -1, 0, 1)


def matmul(left, right):
    return jnp.dot(left, right, preferred_element_type=jnp.float32)


def silu_slope(pre_value):
    sigmoid_v = jax.nn.sigmoid(pre_value)
    return sigmoid_v * (1.0 + pre_value * (1.0 - sigmoid_v))


def fine_forward(owned, ghosts, send_index, recv_index, edge_live, weights):
    w_edge_in, w_edge_out, w_node_in, w_node_out = weights
    latent = owned.shape[1]
    lookup = jnp.concatenate([owned, ghosts], axis=0)
    senders = lookup[send_index]
    receivers = owned[recv_index]
    edge_pre = matmul(senders, w_edge_in[:latent]) + matmul(receivers, w_edge_in[latent:])
    edge_act = jax.nn.silu(edge_pre).astype(jnp.bfloat16)
    message = (matmul(edge_act, w_edge_out) * edge_live[:, None]).astype(jnp.bfloat16)
    summed = jax.ops.segment_sum(message.astype(jnp.float32), recv_index, num_segments=owned.shape[0]).astype(jnp.bfloat16)
    node_pre = matmul(owned, w_node_in[:latent]) + matmul(summed, w_node_in[latent:])
    node_act = jax.nn.silu(node_pre).astype(jnp.bfloat16)
    fine_out = (owned.astype(jnp.float32) + matmul(node_act, w_node_out)).astype(jnp.bfloat16)
    return fine_out, (senders, receivers, edge_pre, edge_act, summed, node_pre, node_act)


def fine_backward(owned, send_index, recv_index, edge_live, weights, stashed, d_total, lookup_rows):
    w_edge_in, w_edge_out, w_node_in, w_node_out = weights
    senders, receivers, edge_pre, edge_act, summed, node_pre, node_act = stashed
    rows_here, latent = owned.shape
    d_out16 = d_total.astype(jnp.bfloat16)
    g_node_out = matmul(node_act.T, d_out16)
    d_node_pre = (matmul(d_out16, w_node_out.T) * silu_slope(node_pre)).astype(jnp.bfloat16)
    g_node_in = jnp.concatenate([matmul(owned.T, d_node_pre), matmul(summed.T, d_node_pre)], axis=0)
    d_owned = d_total + matmul(d_node_pre, w_node_in[:latent].T)
    d_summed = matmul(d_node_pre, w_node_in[latent:].T).astype(jnp.bfloat16)
    d_message = d_summed[recv_index] * edge_live[:, None].astype(d_summed.dtype)
    g_edge_out = matmul(edge_act.T, d_message)
    d_edge_pre = (matmul(d_message, w_edge_out.T) * silu_slope(edge_pre)).astype(jnp.bfloat16)
    g_edge_in = jnp.concatenate([matmul(senders.T, d_edge_pre), matmul(receivers.T, d_edge_pre)], axis=0)
    d_senders = matmul(d_edge_pre, w_edge_in[:latent].T)
    d_receivers = matmul(d_edge_pre, w_edge_in[latent:].T)
    d_lookup = jax.ops.segment_sum(d_senders, send_index, num_segments=lookup_rows)
    d_owned = d_owned + d_lookup[:rows_here] + jax.ops.segment_sum(d_receivers, recv_index, num_segments=rows_here)
    return d_owned, d_lookup[rows_here:], (g_edge_in, g_edge_out, g_node_in, g_node_out)


def reference(nodes, ghost_rows, ghost_count, edge_send, edge_recv, edge_count, pool_map, w_edge_in, w_edge_out, w_node_in, w_node_out, w_coarse_in, w_coarse_out, d_fine, d_coarse):
    devices = N_GX * N_GY
    latent = nodes.shape[1]
    per_device = nodes.reshape(devices, NODE_DEV, latent)
    d_fine_dev = d_fine.reshape(devices, NODE_DEV, latent)
    weights = (w_edge_in, w_edge_out, w_node_in, w_node_out)
    slot_ids = jnp.arange(GBLK, dtype=jnp.int32)
    edge_ids = jnp.arange(EDGE_DEV, dtype=jnp.int32)
    column_ids = jnp.arange(N_GX, dtype=jnp.int32)
    device_ids = jnp.arange(devices, dtype=jnp.int32)
    direction_ids = jnp.arange(8, dtype=jnp.int32)
    across = jnp.array(offset_across, dtype=jnp.int32)
    along = jnp.array(offset_along, dtype=jnp.int32)

    def halo_of(device):
        column_idx = device // N_GY
        row_idx = device % N_GY
        source_column = column_idx - across
        source_row = row_idx - along
        inside = (source_column >= 0) & (source_column < N_GX) & (source_row >= 0) & (source_row < N_GY)
        sources = jnp.clip(source_column, 0, N_GX - 1) * N_GY + jnp.clip(source_row, 0, N_GY - 1)
        ghost_lists = ghost_rows[sources, direction_ids]
        slot_live = (slot_ids[None, :] < ghost_count[sources, direction_ids][:, None]) & inside[:, None]
        picked = per_device[sources[:, None], ghost_lists]
        picked = jnp.where(slot_live[:, :, None], picked, jnp.zeros_like(picked))
        return picked, sources, ghost_lists, slot_live

    def forward_of(device):
        picked, sources, ghost_lists, slot_live = halo_of(device)
        edge_live = (edge_ids < edge_count[device]).astype(jnp.float32)
        return fine_forward(per_device[device], picked.reshape(8 * GBLK, latent), edge_send[device], edge_recv[device], edge_live, weights), edge_live, sources, ghost_lists, slot_live

    fine_all = lax.map(lambda device: forward_of(device)[0][0], device_ids)
    column_rows = N_GY * CO_DEV

    def parents_of(device):
        return pool_map[device] + (device % N_GY) * CO_DEV - BAND

    def pool_column(column_idx):
        members = column_idx * N_GY + jnp.arange(N_GY, dtype=jnp.int32)

        def one_member(values, member):
            return jax.ops.segment_sum(values.astype(jnp.float32), parents_of(member), num_segments=column_rows)

        parts = jax.vmap(one_member)(fine_all[members], members)
        return (0.125 * jnp.sum(parts, axis=0)).astype(jnp.bfloat16)

    coarse_in = lax.map(pool_column, column_ids).reshape(N_GX * column_rows, latent)
    coarse_pre = matmul(coarse_in, w_coarse_in)
    coarse_act = jax.nn.silu(coarse_pre).astype(jnp.bfloat16)
    coarse_out = (coarse_in.astype(jnp.float32) + matmul(coarse_act, w_coarse_out)).astype(jnp.bfloat16)
    g_coarse_out = matmul(coarse_act.T, d_coarse)
    d_coarse_pre = (matmul(d_coarse, w_coarse_out.T) * silu_slope(coarse_pre)).astype(jnp.bfloat16)
    g_coarse_in = matmul(coarse_in.T, d_coarse_pre)
    d_coarse_in = (d_coarse.astype(jnp.float32) + matmul(d_coarse_pre, w_coarse_in.T)).astype(jnp.bfloat16)
    d_column = d_coarse_in.reshape(N_GX, column_rows, latent)

    def backward_step(carry, device):
        grads_nodes, totals = carry
        outcome, edge_live, sources, ghost_lists, slot_live = forward_of(device)
        stashed = outcome[1]
        column_idx = device // N_GY
        d_total = d_fine_dev[device].astype(jnp.float32) + 0.125 * d_column[column_idx][parents_of(device)].astype(jnp.float32)
        d_owned, d_ghosts, partials = fine_backward(per_device[device], edge_send[device], edge_recv[device], edge_live, weights, stashed, d_total, NODE_DEV + 8 * GBLK)
        rounded = lax.optimization_barrier(d_ghosts.astype(jnp.bfloat16)).astype(jnp.float32).reshape(8, GBLK, latent)
        rounded = jnp.where(slot_live[:, :, None], rounded, jnp.zeros_like(rounded))
        grads_nodes = grads_nodes.at[device].add(d_owned)
        grads_nodes = grads_nodes.at[sources[:, None], ghost_lists].add(rounded)
        totals = tuple(total + term for total, term in zip(totals, partials))
        return (grads_nodes, totals), None

    start_totals = (jnp.zeros((2 * latent, HID), jnp.float32), jnp.zeros((HID, latent), jnp.float32), jnp.zeros((2 * latent, HID), jnp.float32), jnp.zeros((HID, latent), jnp.float32))
    start_grads = jnp.zeros((devices, NODE_DEV, latent), jnp.float32)
    (grads_nodes, totals), unused = lax.scan(backward_step, (start_grads, start_totals), device_ids)
    grad_scale = 1.0 / (NODE_DEV * devices) ** 0.5
    return (fine_all.reshape(devices * NODE_DEV, latent), coarse_out, grads_nodes.reshape(devices * NODE_DEV, latent), totals[0] * grad_scale, totals[1] * grad_scale, totals[2] * grad_scale, totals[3] * grad_scale, g_coarse_in * grad_scale, g_coarse_out * grad_scale)
```

```python
import functools

import jax
import jax.numpy as jnp
from jax import lax
from jax.experimental import pallas as pl
from jax.experimental.pallas import tpu as pltpu
from jax.sharding import PartitionSpec as P

BAND = 32
MESH = pl.DeviceIdType.MESH
ACROSS = (-1, -1, -1, 0, 0, 1, 1, 1)
ALONG = (-1, 0, 1, -1, 1, -1, 0, 1)
F32 = jnp.float32
BF16 = jnp.bfloat16
FOLDS = 4


def mm(a, b):
    return jnp.dot(a, b, preferred_element_type=F32)


def mm_t(a, b):
    return lax.dot_general(a, b, (((1,), (1,)), ((), ())), preferred_element_type=F32)


def t_mm(a, b):
    return lax.dot_general(a, b, (((0,), (0,)), ((), ())), preferred_element_type=F32)


def sigmoid(v):
    return 1.0 / (1.0 + jnp.exp(-v))


def pick_lanes(col, width):
    ids = lax.broadcasted_iota(jnp.int32, (col.shape[0], width), 1)
    return jnp.where(ids == col, 1.0, 0.0).astype(BF16)


def pick_sublanes(row, start, height):
    ids = lax.broadcasted_iota(jnp.int32, (height, row.shape[1]), 0)
    return jnp.where(ids == row - start, 1.0, 0.0).astype(BF16)


def fold_of(index, height):
    hi = jnp.zeros_like(index)
    for j in range(1, FOLDS):
        hi = hi + jnp.where(index >= j * height, 1, 0)
    return hi


def gather_folded(col, table):
    height = table.shape[0]
    width = table.shape[1] // FOLDS
    hi = fold_of(col, height)
    wide = mm(pick_lanes(col - hi * height, height), table)
    out = wide[:, :width]
    for j in range(1, FOLDS):
        out = jnp.where(hi == j, wide[:, j * width : (j + 1) * width], out)
    return out


def spread_folds(values, hi):
    values = values.astype(F32)
    return jnp.concatenate(
        [jnp.where(hi == j, values, 0.0).astype(BF16) for j in range(FOLDS)], axis=1
    )


def scatter_folded(row, wide_ref, height, tile, write):
    width = wide_ref.shape[1] // FOLDS
    low = row - fold_of(row, height) * height
    for start in range(0, height, tile):
        sums = mm(pick_sublanes(low, start, tile), wide_ref[...])
        for j in range(FOLDS):
            write(j * height + start, sums[:, j * width : (j + 1) * width])


def write_folded(table, rows, latent):
    height = table.shape[0]
    for j in range(FOLDS):
        table[:, j * latent : (j + 1) * latent] = rows(j * height, height)


def outgoing_kernel(nodes_ref, col_ref, out_ref, table):
    latent = nodes_ref.shape[1]
    write_folded(table, lambda s, h: nodes_ref[s : s + h, :], latent)
    step = 512 if col_ref.shape[0] % 512 == 0 else col_ref.shape[0]
    for s in range(0, col_ref.shape[0], step):
        out_ref[s : s + step, :] = gather_folded(col_ref[s : s + step, :], table[...]).astype(BF16)


def forward_kernel(
    chunk, nodes_ref, ghosts_ref, send_ref, recv_ref, recv_row_ref, pool_row_ref,
    wei_ref, weo_ref, wni_ref, wno_ref,
    fine_ref, window_ref, pre_ref, node_pre_ref, summed_ref,
    lookup, send_table, recv_table, wide,
):
    rows, latent = nodes_ref.shape
    lookup[:rows, :] = nodes_ref[...]
    lookup[rows:, :] = ghosts_ref[...]
    write_folded(send_table, lambda s, h: mm(lookup[s : s + h, :], wei_ref[:latent, :]).astype(BF16), latent)
    write_folded(recv_table, lambda s, h: mm(nodes_ref[s : s + h, :], wei_ref[latent:, :]).astype(BF16), latent)

    def edges(i, carry):
        at = pl.ds(pl.multiple_of(i * chunk, chunk), chunk)
        recv = recv_ref[at, :]
        pre = gather_folded(send_ref[at, :], send_table[...]) + gather_folded(recv, recv_table[...])
        pre_ref[at, :] = pre
        act = (pre * sigmoid(pre)).astype(BF16)
        message = mm(act, weo_ref[...]).astype(BF16)
        wide[at, :] = spread_folds(message, fold_of(recv, rows // FOLDS))
        return carry

    lax.fori_loop(0, send_ref.shape[0] // chunk, edges, 0)

    def put(s, v):
        summed_ref[s : s + v.shape[0], :] = v.astype(BF16)

    scatter_folded(recv_row_ref[...], wide, rows // FOLDS, min(256, rows // FOLDS), put)
    node_pre = mm(nodes_ref[...], wni_ref[:latent, :]) + mm(summed_ref[...], wni_ref[latent:, :])
    node_pre_ref[...] = node_pre
    node_act = (node_pre * sigmoid(node_pre)).astype(BF16)
    fine = (nodes_ref[...].astype(F32) + mm(node_act, wno_ref[...])).astype(BF16)
    fine_ref[...] = fine
    window_ref[...] = mm(pick_sublanes(pool_row_ref[...], 0, window_ref.shape[0]), fine)


def halo_pair(n_gy, low, high, got, send_sem, recv_sem):
    b = lax.axis_index("gy")
    down = pltpu.make_async_remote_copy(
        src_ref=low, dst_ref=got.at[1], send_sem=send_sem.at[0], recv_sem=recv_sem.at[1],
        device_id=(lax.axis_index("gx"), jnp.maximum(b - 1, 0)), device_id_type=MESH)
    up = pltpu.make_async_remote_copy(
        src_ref=high, dst_ref=got.at[0], send_sem=send_sem.at[1], recv_sem=recv_sem.at[0],
        device_id=(lax.axis_index("gx"), jnp.minimum(b + 1, n_gy - 1)), device_id_type=MESH)

    @pl.when(b > 0)
    def _():
        down.start()

    @pl.when(b < n_gy - 1)
    def _():
        up.start()

    @pl.when(b == 0)
    def _():
        got[0] = jnp.zeros(got.shape[1:], got.dtype)

    @pl.when(b == n_gy - 1)
    def _():
        got[1] = jnp.zeros(got.shape[1:], got.dtype)

    @pl.when(b > 0)
    def _():
        down.wait_send()
        up.wait_recv()

    @pl.when(b < n_gy - 1)
    def _():
        up.wait_send()
        down.wait_recv()


def coarse_kernel(
    n_gy, window_ref, d_coarse_ref, wci_ref, wco_ref,
    out_ref, reach_ref, g_in_ref, g_out_ref,
    rims, got_rims, bands, got_bands, send_sem, recv_sem,
):
    co = d_coarse_ref.shape[0]
    a, b = lax.axis_index("gx"), lax.axis_index("gy")
    barrier = pltpu.get_barrier_semaphore()

    @pl.when(b > 0)
    def _():
        pl.semaphore_signal(barrier, inc=1, device_id=(a, jnp.maximum(b - 1, 0)), device_id_type=MESH)

    @pl.when(b < n_gy - 1)
    def _():
        pl.semaphore_signal(barrier, inc=1, device_id=(a, jnp.minimum(b + 1, n_gy - 1)), device_id_type=MESH)

    rims[0] = window_ref[:BAND, :].astype(BF16)
    rims[1] = window_ref[co + BAND :, :].astype(BF16)

    pl.semaphore_wait(barrier, jnp.where(b > 0, 1, 0) + jnp.where(b < n_gy - 1, 1, 0))
    halo_pair(n_gy, rims.at[0], rims.at[1], got_rims, send_sem.at[0], recv_sem.at[0])
    own = window_ref[BAND : co + BAND, :]
    pooled = jnp.concatenate(
        [
            own[:BAND] + got_rims[0].astype(F32),
            own[BAND : co - BAND],
            own[co - BAND :] + got_rims[1].astype(F32),
        ],
        axis=0,
    )
    coarse_in = (0.125 * pooled).astype(BF16)
    d_coarse = d_coarse_ref[...]
    pre = mm(coarse_in, wci_ref[...])
    s = sigmoid(pre)
    d_pre = (mm_t(d_coarse, wco_ref[...]) * (s * (1.0 + pre * (1.0 - s)))).astype(BF16)
    d_in = (d_coarse.astype(F32) + mm_t(d_pre, wci_ref[...])).astype(BF16)
    bands[0] = d_in[:BAND]
    bands[1] = d_in[co - BAND :]
    reach_ref[BAND : co + BAND, :] = d_in
    halo_pair(n_gy, bands.at[0], bands.at[1], got_bands, send_sem.at[1], recv_sem.at[1])
    act = (pre * s).astype(BF16)
    out_ref[...] = (coarse_in.astype(F32) + mm(act, wco_ref[...])).astype(BF16)
    g_out_ref[...] = t_mm(act, d_coarse)
    g_in_ref[...] = t_mm(coarse_in, d_pre)
    reach_ref[:BAND, :] = got_bands[0]
    reach_ref[co + BAND :, :] = got_bands[1]


def backward_kernel(
    chunk, nodes_ref, ghosts_ref, recv_ref, recv_row_ref, send_ref, send_row_ref, pool_ref,
    wei_ref, weo_ref, wni_ref, wno_ref,
    pre_ref, node_pre_ref, summed_ref, reach_ref, d_fine_ref, g_ci_ref, g_co_ref,
    d_owned_ref, d_ghost_ref, g_ref,
    table, recv_wide, send_wide, sums_s, sums_r, g_out,
):
    rows, latent = nodes_ref.shape
    total_rows = rows + ghosts_ref.shape[0]
    nodes = nodes_ref[...]
    d_total = d_fine_ref[...].astype(F32) + 0.125 * mm(
        pick_lanes(pool_ref[...], reach_ref.shape[0]), reach_ref[...]
    )
    d16 = d_total.astype(BF16)
    node_pre = node_pre_ref[...]
    s = sigmoid(node_pre)
    node_act = (node_pre * s).astype(BF16)
    d_node = (mm_t(d16, wno_ref[...]) * (s * (1.0 + node_pre * (1.0 - s)))).astype(BF16)
    base = 2 * latent
    g_ref[base + latent : base + 2 * latent, :] = t_mm(nodes, d_node)
    g_ref[base + 2 * latent : base + 3 * latent, :] = t_mm(summed_ref[...], d_node)
    g_ref[base + 3 * latent : base + 4 * latent, :] = t_mm(node_act, d16)
    g_ref[base + 4 * latent : base + 5 * latent, :] = g_ci_ref[...]
    g_ref[base + 5 * latent : base + 6 * latent, :] = g_co_ref[...]
    d_owned_ref[...] = d_total + mm_t(d_node, wni_ref[:latent, :])
    d_summed = mm_t(d_node, wni_ref[latent:, :]).astype(BF16)
    height = rows // FOLDS
    for j in range(FOLDS):
        table[:, j * latent : (j + 1) * latent] = d_summed[j * height : (j + 1) * height]
    g_out[...] = jnp.zeros_like(g_out)

    def edges(i, carry):
        at = pl.ds(pl.multiple_of(i * chunk, chunk), chunk)
        recv = recv_ref[at, :]
        d_message = gather_folded(recv, table[...]).astype(BF16)
        pre = pre_ref[at, :]
        sig = sigmoid(pre)
        act = (pre * sig).astype(BF16)
        g_out[...] += t_mm(act, d_message)
        d_pre = (mm_t(d_message, weo_ref[...]) * (sig * (1.0 + pre * (1.0 - sig)))).astype(BF16)
        recv_wide[at, :] = spread_folds(d_pre, fold_of(recv, height))
        send_wide[at, :] = spread_folds(d_pre, fold_of(send_ref[at, :], total_rows // FOLDS))
        return carry

    lax.fori_loop(0, send_ref.shape[0] // chunk, edges, 0)
    g_ref[base : base + latent, :] = g_out[...]

    def put_s(at, v):
        sums_s[at : at + v.shape[0], :] = v.astype(BF16)

    def put_r(at, v):
        sums_r[at : at + v.shape[0], :] = v.astype(BF16)

    scatter_folded(recv_row_ref[...], recv_wide, height, min(256, height), put_r)
    scatter_folded(send_row_ref[...], send_wide, total_rows // FOLDS, min(256, total_rows // FOLDS), put_s)
    w_send, w_recv = wei_ref[:latent, :], wei_ref[latent:, :]
    d_owned_ref[...] += mm_t(sums_s[:rows, :], w_send) + mm_t(sums_r[...], w_recv)
    d_ghost_ref[...] = mm_t(sums_s[rows:, :], w_send).astype(BF16)
    g_ref[:latent, :] = t_mm(nodes, sums_s[:rows, :]) + t_mm(ghosts_ref[...], sums_s[rows:, :])
    g_ref[latent:base, :] = t_mm(nodes, sums_r[...])


def neighbours(n_gx, n_gy, sign):
    a, b = lax.axis_index("gx"), lax.axis_index("gy")
    found = []
    for dx, dy in zip(ACROSS, ALONG):
        dx, dy = sign * dx, sign * dy
        ta, tb = a + dx, b + dy
        sa, sb = a - dx, b - dy
        there = (ta >= 0) & (ta < n_gx) & (tb >= 0) & (tb < n_gy)
        here = (sa >= 0) & (sa < n_gx) & (sb >= 0) & (sb < n_gy)
        target = (jnp.clip(ta, 0, n_gx - 1), jnp.clip(tb, 0, n_gy - 1))
        found.append((target, there, here))
    return found


def greet(barrier, found):
    for target, there, _ in found:
        @pl.when(there)
        def _(target=target):
            pl.semaphore_signal(barrier, inc=1, device_id=target, device_id_type=MESH)


def greeted(barrier, found, more=0):
    count = jnp.int32(more)
    for _, there, _ in found:
        count = count + jnp.where(there, 1, 0)
    pl.semaphore_wait(barrier, count)


def exchange_copies(found, src_ref, dst_ref, send_sem, recv_sem):
    return [
        pltpu.make_async_remote_copy(
            src_ref=src_ref.at[k], dst_ref=dst_ref.at[k], send_sem=send_sem.at[k],
            recv_sem=recv_sem.at[k], device_id=found[k][0], device_id_type=MESH)
        for k in range(len(found))
    ]


def exchange_start(found, copies, dst_ref):
    for k in range(len(found)):
        @pl.when(found[k][1])
        def _(k=k):
            copies[k].start()

    for k in range(len(found)):
        @pl.when(jnp.logical_not(found[k][2]))
        def _(k=k):
            dst_ref[k] = jnp.zeros(dst_ref.shape[1:], dst_ref.dtype)


def exchange_wait(found, copies):
    for k in range(len(found)):
        @pl.when(found[k][1])
        def _(k=k):
            copies[k].wait_send()

        @pl.when(found[k][2])
        def _(k=k):
            copies[k].wait_recv()


def exchange_kernel(n_gx, n_gy, src_ref, dst_ref, send_sem, recv_sem):
    found = neighbours(n_gx, n_gy, 1)
    barrier = pltpu.get_barrier_semaphore()
    greet(barrier, found)
    greeted(barrier, found)
    copies = exchange_copies(found, src_ref, dst_ref, send_sem, recv_sem)
    exchange_start(found, copies, dst_ref)
    exchange_wait(found, copies)


def reduce_kernel(
    n_gx, n_gy, ghost_ref, g_ref, back_ref, total_ref,
    g16, got_x, mid, got_y, ghost_send, ghost_recv, xs, xr, ys, yr, xs2, xr2, ys2, yr2,
):
    a, b = lax.axis_index("gx"), lax.axis_index("gy")
    found = neighbours(n_gx, n_gy, -1)
    peers_x = [(lax.rem(a + r, n_gx), b) for r in range(1, n_gx)]
    peers_y = [(a, lax.rem(b + r, n_gy)) for r in range(1, n_gy)]
    barrier = pltpu.get_barrier_semaphore()
    corners = [f for f, dx, dy in zip(found, ACROSS, ALONG) if dx and dy]
    greet(barrier, corners)
    for peer in peers_x + peers_y:
        pl.semaphore_signal(barrier, inc=1, device_id=peer, device_id_type=MESH)
    g16[...] = g_ref[...].astype(BF16)
    greeted(barrier, corners, n_gx + n_gy - 2)

    def remote(src, dst, send, recv, peer):
        return pltpu.make_async_remote_copy(
            src_ref=src, dst_ref=dst, send_sem=send, recv_sem=recv, device_id=peer, device_id_type=MESH)

    first = [
        remote(g16.at[p[0]], got_x.at[r], xs.at[r], xr.at[r], p) for r, p in enumerate(peers_x)
    ]
    for copy in first:
        copy.start()
    copies = exchange_copies(found, ghost_ref, back_ref, ghost_send, ghost_recv)
    exchange_start(found, copies, back_ref)
    total = g_ref[a]
    for r, copy in enumerate(first):
        copy.wait_recv()
        total = total + got_x[r].astype(F32)
    mid[...] = total.astype(BF16)
    second = [
        remote(mid.at[p[1]], got_y.at[r], ys.at[r], yr.at[r], p) for r, p in enumerate(peers_y)
    ]
    for copy in second:
        copy.start()
    final = mid[b].astype(F32)
    for r, copy in enumerate(second):
        copy.wait_recv()
        final = final + got_y[r].astype(F32)
    total_ref[a, b] = final.astype(BF16)
    third = [
        remote(total_ref.at[a, b], total_ref.at[a, b], ys2.at[r], yr2.at[r], p) for r, p in enumerate(peers_y)
    ]
    for copy in third:
        copy.start()
    for copy in third:
        copy.wait_recv()
    fourth = [
        remote(total_ref.at[a], total_ref.at[a], xs2.at[r], xr2.at[r], p) for r, p in enumerate(peers_x)
    ]
    for copy in fourth:
        copy.start()
    for copy in fourth:
        copy.wait_recv()
    exchange_wait(found, copies)
    for copy in first + second + third + fourth:
        copy.wait_send()


def final_kernel(
    scale, d_owned_ref, back_ref, col_ref, row_ref, total_ref,
    nodes_out, ei_ref, eo_ref, ni_ref, no_ref, ci_ref, co_ref, wide,
):
    height = d_owned_ref.shape[0] // FOLDS
    wide[...] = spread_folds(back_ref[...], fold_of(col_ref[...], height))

    def put(at, v):
        nodes_out[at : at + v.shape[0], :] = d_owned_ref[at : at + v.shape[0], :] + v

    scatter_folded(row_ref[...], wide, height, min(256, height), put)
    at = 0
    for ref in (ei_ref, eo_ref, ni_ref, no_ref, ci_ref, co_ref):
        ref[...] = total_ref[at : at + ref.shape[0], :].astype(F32) * scale
        at += ref.shape[0]


def call(kernel, outs, scratch, args, collective_id=None):
    extra = {}
    if collective_id is not None:
        extra = dict(collective_id=collective_id, has_side_effects=True)
    vmem = pl.BlockSpec(memory_space=pltpu.VMEM)
    return pl.pallas_call(
        kernel,
        out_shape=[jax.ShapeDtypeStruct(shape, kind) for shape, kind in outs],
        in_specs=[vmem] * len(args),
        out_specs=[vmem] * len(outs),
        scratch_shapes=scratch,
        compiler_params=pltpu.CompilerParams(vmem_limit_bytes=56 * 1024 * 1024, **extra),
    )(*args)


def body(
    n_gx, n_gy, nodes, ghost_rows, ghost_count, edge_send, edge_recv, edge_count, pool_map,
    w_edge_in, w_edge_out, w_node_in, w_node_out, w_coarse_in, w_coarse_out, d_fine, d_coarse,
):
    rows, latent = nodes.shape
    _, peers, slots = ghost_rows.shape
    ghosts_n = peers * slots
    edges_n = edge_send.shape[1]
    co = d_coarse.shape[0]
    chunk = 512 if edges_n % 512 == 0 else edges_n
    dma = pltpu.SemaphoreType.DMA
    live = jnp.arange(slots, dtype=jnp.int32)[None, :] < ghost_count[0][:, None]
    ghost_index = jnp.where(live, ghost_rows[0], -1).reshape(1, ghosts_n)
    ghost_col = ghost_index.reshape(ghosts_n, 1)
    edge_live = jnp.arange(edges_n, dtype=jnp.int32) < edge_count[0]
    recv_row = jnp.where(edge_live, edge_recv[0], -1).reshape(1, edges_n)
    recv_col = recv_row.reshape(edges_n, 1)
    send_row = edge_send
    send_col = edge_send.reshape(edges_n, 1)
    pool_col = pool_map.reshape(rows, 1)
    fold_rows = rows // FOLDS
    fold_all = (rows + ghosts_n) // FOLDS

    (outgoing,) = call(
        outgoing_kernel, [((ghosts_n, latent), BF16)],
        [pltpu.VMEM((fold_rows, FOLDS * latent), BF16)], (nodes, ghost_col))
    (arrived,) = call(
        functools.partial(exchange_kernel, n_gx, n_gy), [((peers, slots, latent), BF16)],
        [dma((peers,)), dma((peers,))], (outgoing.reshape(peers, slots, latent),), 0)
    ghosts = arrived.reshape(ghosts_n, latent)
    fine_out, window, pre, node_pre, summed = call(
        functools.partial(forward_kernel, chunk),
        [((rows, latent), BF16), ((co + 2 * BAND, latent), F32), ((edges_n, latent), F32),
         ((rows, latent), F32), ((rows, latent), BF16)],
        [pltpu.VMEM((rows + ghosts_n, latent), BF16), pltpu.VMEM((fold_all, FOLDS * latent), BF16),
         pltpu.VMEM((fold_rows, FOLDS * latent), BF16), pltpu.VMEM((edges_n, FOLDS * latent), BF16)],
        (nodes, ghosts, send_col, recv_col, recv_row, pool_map, w_edge_in, w_edge_out, w_node_in, w_node_out))
    coarse_out, reach, g_ci, g_co = call(
        functools.partial(coarse_kernel, n_gy),
        [((co, latent), BF16), ((co + 2 * BAND, latent), BF16), ((latent, latent), F32), ((latent, latent), F32)],
        [pltpu.VMEM((2, BAND, latent), BF16)] * 4 + [dma((2, 2)), dma((2, 2))],
        (window, d_coarse, w_coarse_in, w_coarse_out), 1)
    d_owned, d_ghosts, partial = call(
        functools.partial(backward_kernel, chunk),
        [((rows, latent), F32), ((ghosts_n, latent), BF16), ((8 * latent, latent), F32)],
        [pltpu.VMEM((fold_rows, FOLDS * latent), BF16), pltpu.VMEM((edges_n, FOLDS * latent), BF16),
         pltpu.VMEM((edges_n, FOLDS * latent), BF16), pltpu.VMEM((rows + ghosts_n, latent), BF16),
         pltpu.VMEM((rows, latent), BF16), pltpu.VMEM((latent, latent), F32)],
        (nodes, ghosts, recv_col, recv_row, send_col, send_row, pool_col, w_edge_in, w_edge_out, w_node_in,
         w_node_out, pre, node_pre, summed, reach, d_fine, g_ci, g_co))
    share = 8 * latent // (n_gx * n_gy)
    parts = (n_gx, n_gy, share, latent)
    back, total = call(
        functools.partial(reduce_kernel, n_gx, n_gy),
        [((peers, slots, latent), BF16), (parts, BF16)],
        [pltpu.VMEM(parts, BF16), pltpu.VMEM((n_gx - 1,) + parts[1:], BF16), pltpu.VMEM(parts[1:], BF16),
         pltpu.VMEM((n_gy - 1,) + parts[2:], BF16), dma((peers,)), dma((peers,))]
        + [dma((n_gx - 1,))] * 2 + [dma((n_gy - 1,))] * 2 + [dma((n_gx - 1,))] * 2 + [dma((n_gy - 1,))] * 2,
        (d_ghosts.reshape(peers, slots, latent), partial.reshape(parts)), 2)
    scale = 1.0 / (rows * n_gx * n_gy) ** 0.5
    outs = call(
        functools.partial(final_kernel, scale),
        [((rows, latent), F32), ((2 * latent, latent), F32), ((latent, latent), F32), ((2 * latent, latent), F32),
         ((latent, latent), F32), ((latent, latent), F32), ((latent, latent), F32)],
        [pltpu.VMEM((ghosts_n, FOLDS * latent), BF16)],
        (d_owned, back.reshape(ghosts_n, latent), ghost_col, ghost_index, total.reshape(8 * latent, latent)))
    return (fine_out, coarse_out) + tuple(outs)


def solution(mesh):
    split = P(("gx", "gy"), None)
    return jax.shard_map(
        functools.partial(body, mesh.shape["gx"], mesh.shape["gy"]),
        mesh=mesh,
        in_specs=(split, P(("gx", "gy"), None, None), split, split, split, P(("gx", "gy")), split)
        + (P(),) * 6
        + (split, split),
        out_specs=(split, split, split) + (P(),) * 6,
        check_vma=False,
    )
```

```python
import functools

import jax
import jax.numpy as jnp
from jax import lax
from jax.experimental import pallas as pl
from jax.experimental.pallas import tpu as pltpu
from jax.sharding import PartitionSpec as P

BAND = 32
MESH = pl.DeviceIdType.MESH
ACROSS = (-1, -1, -1, 0, 0, 1, 1, 1)
ALONG = (-1, 0, 1, -1, 1, -1, 0, 1)
SEND_ORDER = (0, 2, 5, 7, 3, 4, 1, 6)
F32 = jnp.float32
BF16 = jnp.bfloat16
FOLDS = 4
LANES = 128


def mm(a, b):
    return jnp.dot(a, b, preferred_element_type=F32)


def mm_t(a, b):
    return lax.dot_general(a, b, (((1,), (1,)), ((), ())), preferred_element_type=F32)


def t_mm(a, b):
    return lax.dot_general(a, b, (((0,), (0,)), ((), ())), preferred_element_type=F32)


def sigmoid(v):
    return 1.0 / (1.0 + jnp.exp(-v))


def columns(row):
    return jnp.concatenate(
        [
            jnp.transpose(jnp.broadcast_to(row[:, s : s + LANES], (LANES, LANES)))
            for s in range(0, row.shape[1], LANES)
        ],
        axis=0,
    )


def alive(row, start, count):
    ids = lax.broadcasted_iota(jnp.int32, row.shape, 1) + start
    return jnp.where(ids < count, row, -1)


def pick_lanes(col, width):
    ids = lax.broadcasted_iota(jnp.int32, (col.shape[0], LANES), 1)
    parts = [
        jnp.where(ids == col - s, 1.0, 0.0).astype(BF16)[:, : min(LANES, width - s)]
        for s in range(0, width, LANES)
    ]
    return jnp.concatenate(parts, axis=1)


def pick_sublanes(row, start, height):
    ids = lax.broadcasted_iota(jnp.int32, (height, row.shape[1]), 0)
    return jnp.where(ids == row - start, 1.0, 0.0).astype(BF16)


def fold_of(index, height):
    hi = jnp.zeros_like(index)
    for j in range(1, FOLDS):
        hi = hi + jnp.where(index >= j * height, 1, 0)
    return hi


def gather_folded(col, table):
    height = table.shape[0]
    width = table.shape[1] // FOLDS
    hi = fold_of(col, height)
    wide = mm(pick_lanes(col - hi * height, height), table)
    out = wide[:, :width]
    for j in range(1, FOLDS):
        out = jnp.where(hi == j, wide[:, j * width : (j + 1) * width], out)
    return out


def spread_folds(values, hi):
    values = values.astype(F32)
    return jnp.concatenate(
        [jnp.where(hi == j, values, 0.0).astype(BF16) for j in range(FOLDS)], axis=1
    )


def scatter_folded(row, wide_ref, height, tile, write):
    width = wide_ref.shape[1] // FOLDS
    low = row - fold_of(row, height) * height
    for start in range(0, height, tile):
        sums = mm(pick_sublanes(low, start, tile), wide_ref[...])
        for j in range(FOLDS):
            write(j * height + start, sums[:, j * width : (j + 1) * width])


def write_folded(table, rows, latent):
    height = table.shape[0]
    for j in range(FOLDS):
        table[:, j * latent : (j + 1) * latent] = rows(j * height, height)


def forward_kernel(
    chunk, nodes_ref, ghosts_ref, send_ref, recv_ref, count_ref, pool_row_ref,
    wei_ref, weo_ref, wni_ref, wno_ref,
    fine_ref, window_ref, pre_ref, node_pre_ref, summed_ref,
    lookup, send_table, recv_table, wide,
):
    rows, latent = nodes_ref.shape
    lookup[:rows, :] = nodes_ref[...]
    lookup[rows:, :] = ghosts_ref[...]
    write_folded(send_table, lambda s, h: mm(lookup[s : s + h, :], wei_ref[:latent, :]).astype(BF16), latent)
    write_folded(recv_table, lambda s, h: mm(nodes_ref[s : s + h, :], wei_ref[latent:, :]).astype(BF16), latent)

    def edges(i, carry):
        at = pl.ds(pl.multiple_of(i * chunk, chunk), chunk)
        recv = columns(alive(recv_ref[:, at], i * chunk, count_ref[...]))
        pre = gather_folded(columns(send_ref[:, at]), send_table[...]) + gather_folded(recv, recv_table[...])
        pre_ref[at, :] = pre
        act = (pre * sigmoid(pre)).astype(BF16)
        message = mm(act, weo_ref[...]).astype(BF16)
        wide[at, :] = spread_folds(message, fold_of(recv, rows // FOLDS))
        return carry

    lax.fori_loop(0, send_ref.shape[1] // chunk, edges, 0)

    def put(s, v):
        summed_ref[s : s + v.shape[0], :] = v.astype(BF16)

    scatter_folded(alive(recv_ref[...], 0, count_ref[...]), wide, rows // FOLDS, min(256, rows // FOLDS), put)
    node_pre = mm(nodes_ref[...], wni_ref[:latent, :]) + mm(summed_ref[...], wni_ref[latent:, :])
    node_pre_ref[...] = node_pre
    node_act = (node_pre * sigmoid(node_pre)).astype(BF16)
    fine = (nodes_ref[...].astype(F32) + mm(node_act, wno_ref[...])).astype(BF16)
    fine_ref[...] = fine
    window_ref[...] = mm(pick_sublanes(pool_row_ref[...], 0, window_ref.shape[0]), fine)


def halo_pair(n_gy, low, high, got, send_sem, recv_sem):
    b = lax.axis_index("gy")
    down = pltpu.make_async_remote_copy(
        src_ref=low, dst_ref=got.at[1], send_sem=send_sem.at[0], recv_sem=recv_sem.at[1],
        device_id=(lax.axis_index("gx"), jnp.maximum(b - 1, 0)), device_id_type=MESH)
    up = pltpu.make_async_remote_copy(
        src_ref=high, dst_ref=got.at[0], send_sem=send_sem.at[1], recv_sem=recv_sem.at[0],
        device_id=(lax.axis_index("gx"), jnp.minimum(b + 1, n_gy - 1)), device_id_type=MESH)

    @pl.when(b > 0)
    def _():
        down.start()

    @pl.when(b < n_gy - 1)
    def _():
        up.start()

    @pl.when(b == 0)
    def _():
        got[0] = jnp.zeros(got.shape[1:], got.dtype)

    @pl.when(b == n_gy - 1)
    def _():
        got[1] = jnp.zeros(got.shape[1:], got.dtype)

    @pl.when(b > 0)
    def _():
        down.wait_send()
        up.wait_recv()

    @pl.when(b < n_gy - 1)
    def _():
        up.wait_send()
        down.wait_recv()


def coarse_kernel(
    n_gy, window_ref, d_coarse_ref, wci_ref, wco_ref,
    out_ref, reach_ref, g_in_ref, g_out_ref,
    rims, got_rims, bands, got_bands, send_sem, recv_sem,
):
    co = d_coarse_ref.shape[0]
    a, b = lax.axis_index("gx"), lax.axis_index("gy")
    barrier = pltpu.get_barrier_semaphore()

    @pl.when(b > 0)
    def _():
        pl.semaphore_signal(barrier, inc=1, device_id=(a, jnp.maximum(b - 1, 0)), device_id_type=MESH)

    @pl.when(b < n_gy - 1)
    def _():
        pl.semaphore_signal(barrier, inc=1, device_id=(a, jnp.minimum(b + 1, n_gy - 1)), device_id_type=MESH)

    rims[0] = window_ref[:BAND, :].astype(BF16)
    rims[1] = window_ref[co + BAND :, :].astype(BF16)

    pl.semaphore_wait(barrier, jnp.where(b > 0, 1, 0) + jnp.where(b < n_gy - 1, 1, 0))
    halo_pair(n_gy, rims.at[0], rims.at[1], got_rims, send_sem.at[0], recv_sem.at[0])
    own = window_ref[BAND : co + BAND, :]
    pooled = jnp.concatenate(
        [
            own[:BAND] + got_rims[0].astype(F32),
            own[BAND : co - BAND],
            own[co - BAND :] + got_rims[1].astype(F32),
        ],
        axis=0,
    )
    coarse_in = (0.125 * pooled).astype(BF16)
    d_coarse = d_coarse_ref[...]
    pre = mm(coarse_in, wci_ref[...])
    s = sigmoid(pre)
    d_pre = (mm_t(d_coarse, wco_ref[...]) * (s * (1.0 + pre * (1.0 - s)))).astype(BF16)
    d_in = (d_coarse.astype(F32) + mm_t(d_pre, wci_ref[...])).astype(BF16)
    bands[0] = d_in[:BAND]
    bands[1] = d_in[co - BAND :]
    reach_ref[BAND : co + BAND, :] = d_in
    halo_pair(n_gy, bands.at[0], bands.at[1], got_bands, send_sem.at[1], recv_sem.at[1])
    act = (pre * s).astype(BF16)
    out_ref[...] = (coarse_in.astype(F32) + mm(act, wco_ref[...])).astype(BF16)
    g_out_ref[...] = t_mm(act, d_coarse)
    g_in_ref[...] = t_mm(coarse_in, d_pre)
    reach_ref[:BAND, :] = got_bands[0]
    reach_ref[co + BAND :, :] = got_bands[1]


def backward_kernel(
    chunk, nodes_ref, ghosts_ref, recv_ref, count_ref, send_ref, pool_ref,
    wei_ref, weo_ref, wni_ref, wno_ref,
    pre_ref, node_pre_ref, summed_ref, reach_ref, d_fine_ref, g_ci_ref, g_co_ref,
    d_owned_ref, d_ghost_ref, g_ref,
    table, recv_wide, send_wide, sums_s, sums_r, g_out,
):
    rows, latent = nodes_ref.shape
    total_rows = rows + ghosts_ref.shape[0]
    nodes = nodes_ref[...]
    d_total = d_fine_ref[...].astype(F32) + 0.125 * mm(
        pick_lanes(columns(pool_ref[...]), reach_ref.shape[0]), reach_ref[...]
    )
    d16 = d_total.astype(BF16)
    node_pre = node_pre_ref[...]
    s = sigmoid(node_pre)
    node_act = (node_pre * s).astype(BF16)
    d_node = (mm_t(d16, wno_ref[...]) * (s * (1.0 + node_pre * (1.0 - s)))).astype(BF16)
    base = 2 * latent
    g_ref[base + latent : base + 2 * latent, :] = t_mm(nodes, d_node)
    g_ref[base + 2 * latent : base + 3 * latent, :] = t_mm(summed_ref[...], d_node)
    g_ref[base + 3 * latent : base + 4 * latent, :] = t_mm(node_act, d16)
    g_ref[base + 4 * latent : base + 5 * latent, :] = g_ci_ref[...]
    g_ref[base + 5 * latent : base + 6 * latent, :] = g_co_ref[...]
    d_owned_ref[...] = d_total + mm_t(d_node, wni_ref[:latent, :])
    d_summed = mm_t(d_node, wni_ref[latent:, :]).astype(BF16)
    height = rows // FOLDS
    for j in range(FOLDS):
        table[:, j * latent : (j + 1) * latent] = d_summed[j * height : (j + 1) * height]
    g_out[...] = jnp.zeros_like(g_out)

    def edges(i, carry):
        at = pl.ds(pl.multiple_of(i * chunk, chunk), chunk)
        recv = columns(alive(recv_ref[:, at], i * chunk, count_ref[...]))
        d_message = gather_folded(recv, table[...]).astype(BF16)
        pre = pre_ref[at, :]
        sig = sigmoid(pre)
        act = (pre * sig).astype(BF16)
        g_out[...] += t_mm(act, d_message)
        d_pre = (mm_t(d_message, weo_ref[...]) * (sig * (1.0 + pre * (1.0 - sig)))).astype(BF16)
        recv_wide[at, :] = spread_folds(d_pre, fold_of(recv, height))
        send_wide[at, :] = spread_folds(d_pre, fold_of(columns(send_ref[:, at]), total_rows // FOLDS))
        return carry

    lax.fori_loop(0, send_ref.shape[1] // chunk, edges, 0)
    g_ref[base : base + latent, :] = g_out[...]

    def put_s(at, v):
        sums_s[at : at + v.shape[0], :] = v.astype(BF16)

    def put_r(at, v):
        sums_r[at : at + v.shape[0], :] = v.astype(BF16)

    scatter_folded(alive(recv_ref[...], 0, count_ref[...]), recv_wide, height, min(256, height), put_r)
    scatter_folded(send_ref[...], send_wide, total_rows // FOLDS, min(256, total_rows // FOLDS), put_s)
    w_send, w_recv = wei_ref[:latent, :], wei_ref[latent:, :]
    d_owned_ref[...] += mm_t(sums_s[:rows, :], w_send) + mm_t(sums_r[...], w_recv)
    d_ghost_ref[...] = mm_t(sums_s[rows:, :], w_send).astype(BF16)
    g_ref[:latent, :] = t_mm(nodes, sums_s[:rows, :]) + t_mm(ghosts_ref[...], sums_s[rows:, :])
    g_ref[latent:base, :] = t_mm(nodes, sums_r[...])


def neighbours(n_gx, n_gy, sign):
    a, b = lax.axis_index("gx"), lax.axis_index("gy")
    found = []
    for dx, dy in zip(ACROSS, ALONG):
        dx, dy = sign * dx, sign * dy
        ta, tb = a + dx, b + dy
        sa, sb = a - dx, b - dy
        there = (ta >= 0) & (ta < n_gx) & (tb >= 0) & (tb < n_gy)
        here = (sa >= 0) & (sa < n_gx) & (sb >= 0) & (sb < n_gy)
        target = (jnp.clip(ta, 0, n_gx - 1), jnp.clip(tb, 0, n_gy - 1))
        found.append((target, there, here))
    return found


def greet(barrier, found):
    for target, there, _ in found:
        @pl.when(there)
        def _(target=target):
            pl.semaphore_signal(barrier, inc=1, device_id=target, device_id_type=MESH)


def greeted(barrier, found, more=0):
    count = jnp.int32(more)
    for _, there, _ in found:
        count = count + jnp.where(there, 1, 0)
    pl.semaphore_wait(barrier, count)


def exchange_copies(found, src_ref, dst_ref, send_sem, recv_sem):
    return [
        pltpu.make_async_remote_copy(
            src_ref=src_ref.at[k], dst_ref=dst_ref.at[k], send_sem=send_sem.at[k],
            recv_sem=recv_sem.at[k], device_id=found[k][0], device_id_type=MESH)
        for k in range(len(found))
    ]


def exchange_start(found, copies, dst_ref):
    for k in range(len(found)):
        @pl.when(found[k][1])
        def _(k=k):
            copies[k].start()

    for k in range(len(found)):
        @pl.when(jnp.logical_not(found[k][2]))
        def _(k=k):
            dst_ref[k] = jnp.zeros(dst_ref.shape[1:], dst_ref.dtype)


def exchange_wait(found, copies):
    for k in range(len(found)):
        @pl.when(found[k][1])
        def _(k=k):
            copies[k].wait_send()

        @pl.when(found[k][2])
        def _(k=k):
            copies[k].wait_recv()


def ghost_row(rows_ref, count_ref, k):
    return alive(rows_ref[0, k : k + 1, :], 0, count_ref[:, k : k + 1])


def exchange_kernel(n_gx, n_gy, nodes_ref, rows_ref, count_ref, dst_ref, table, outgoing, send_sem, recv_sem):
    found = neighbours(n_gx, n_gy, 1)
    barrier = pltpu.get_barrier_semaphore()
    greet(barrier, found)
    write_folded(table, lambda s, h: nodes_ref[s : s + h, :], nodes_ref.shape[1])
    copies = exchange_copies(found, outgoing, dst_ref, send_sem, recv_sem)
    for n, k in enumerate(SEND_ORDER):
        outgoing[k] = gather_folded(columns(ghost_row(rows_ref, count_ref, k)), table[...]).astype(BF16)
        if n == 0:
            greeted(barrier, found)

        @pl.when(found[k][1])
        def _(k=k):
            copies[k].start()

    for k in range(len(found)):
        @pl.when(jnp.logical_not(found[k][2]))
        def _(k=k):
            dst_ref[k] = jnp.zeros(dst_ref.shape[1:], dst_ref.dtype)

    exchange_wait(found, copies)


def reduce_kernel(
    n_gx, n_gy, ghost_ref, g_ref, back_ref, total_ref,
    g16, got_x, mid, got_y, ghost_send, ghost_recv, xs, xr, ys, yr, xs2, xr2, ys2, yr2,
):
    a, b = lax.axis_index("gx"), lax.axis_index("gy")
    found = neighbours(n_gx, n_gy, -1)
    peers_x = [(lax.rem(a + r, n_gx), b) for r in range(1, n_gx)]
    peers_y = [(a, lax.rem(b + r, n_gy)) for r in range(1, n_gy)]
    barrier = pltpu.get_barrier_semaphore()
    corners = [f for f, dx, dy in zip(found, ACROSS, ALONG) if dx and dy]
    greet(barrier, corners)
    for peer in peers_x + peers_y:
        pl.semaphore_signal(barrier, inc=1, device_id=peer, device_id_type=MESH)
    g16[...] = g_ref[...].astype(BF16)
    greeted(barrier, corners, n_gx + n_gy - 2)

    def remote(src, dst, send, recv, peer):
        return pltpu.make_async_remote_copy(
            src_ref=src, dst_ref=dst, send_sem=send, recv_sem=recv, device_id=peer, device_id_type=MESH)

    first = [
        remote(g16.at[p[0]], got_x.at[r], xs.at[r], xr.at[r], p) for r, p in enumerate(peers_x)
    ]
    for copy in first:
        copy.start()
    copies = exchange_copies(found, ghost_ref, back_ref, ghost_send, ghost_recv)
    exchange_start(found, copies, back_ref)
    total = g_ref[a]
    for r, copy in enumerate(first):
        copy.wait_recv()
        total = total + got_x[r].astype(F32)
    mid[...] = total.astype(BF16)
    second = [
        remote(mid.at[p[1]], got_y.at[r], ys.at[r], yr.at[r], p) for r, p in enumerate(peers_y)
    ]
    for copy in second:
        copy.start()
    final = mid[b].astype(F32)
    for r, copy in enumerate(second):
        copy.wait_recv()
        final = final + got_y[r].astype(F32)
    total_ref[a, b] = final.astype(BF16)
    third = [
        remote(total_ref.at[a, b], total_ref.at[a, b], ys2.at[r], yr2.at[r], p) for r, p in enumerate(peers_y)
    ]
    for copy in third:
        copy.start()
    for copy in third:
        copy.wait_recv()
    fourth = [
        remote(total_ref.at[a], total_ref.at[a], xs2.at[r], xr2.at[r], p) for r, p in enumerate(peers_x)
    ]
    for copy in fourth:
        copy.start()
    for copy in fourth:
        copy.wait_recv()
    exchange_wait(found, copies)
    for copy in first + second + third + fourth:
        copy.wait_send()


def final_kernel(
    scale, d_owned_ref, back_ref, rows_ref, count_ref, total_ref,
    nodes_out, ei_ref, eo_ref, ni_ref, no_ref, ci_ref, co_ref, wide,
):
    height = d_owned_ref.shape[0] // FOLDS
    index = [ghost_row(rows_ref, count_ref, k) for k in range(rows_ref.shape[1])]
    for k, row in enumerate(index):
        wide[k * row.shape[1] : (k + 1) * row.shape[1], :] = spread_folds(
            back_ref[k], fold_of(columns(row), height)
        )

    def put(at, v):
        nodes_out[at : at + v.shape[0], :] = d_owned_ref[at : at + v.shape[0], :] + v

    scatter_folded(jnp.concatenate(index, axis=1), wide, height, min(256, height), put)
    at = 0
    for ref in (ei_ref, eo_ref, ni_ref, no_ref, ci_ref, co_ref):
        ref[...] = total_ref[at : at + ref.shape[0], :].astype(F32) * scale
        at += ref.shape[0]


def call(kernel, outs, scratch, args, collective_id=None):
    extra = {}
    if collective_id is not None:
        extra = dict(collective_id=collective_id, has_side_effects=True)
    vmem = pl.BlockSpec(memory_space=pltpu.VMEM)
    return pl.pallas_call(
        kernel,
        out_shape=[jax.ShapeDtypeStruct(shape, kind) for shape, kind in outs],
        in_specs=[vmem] * len(args),
        out_specs=[vmem] * len(outs),
        scratch_shapes=scratch,
        compiler_params=pltpu.CompilerParams(vmem_limit_bytes=56 * 1024 * 1024, **extra),
    )(*args)


def body(
    n_gx, n_gy, nodes, ghost_rows, ghost_count, edge_send, edge_recv, edge_count, pool_map,
    w_edge_in, w_edge_out, w_node_in, w_node_out, w_coarse_in, w_coarse_out, d_fine, d_coarse,
):
    rows, latent = nodes.shape
    _, peers, slots = ghost_rows.shape
    ghosts_n = peers * slots
    edges_n = edge_send.shape[1]
    co = d_coarse.shape[0]
    chunk = 512 if edges_n % 512 == 0 else edges_n
    dma = pltpu.SemaphoreType.DMA
    edge_total = edge_count.reshape(1, 1)
    fold_rows = rows // FOLDS
    fold_all = (rows + ghosts_n) // FOLDS

    (arrived,) = call(
        functools.partial(exchange_kernel, n_gx, n_gy), [((peers, slots, latent), BF16)],
        [pltpu.VMEM((fold_rows, FOLDS * latent), BF16), pltpu.VMEM((peers, slots, latent), BF16),
         dma((peers,)), dma((peers,))], (nodes, ghost_rows, ghost_count), 0)
    ghosts = arrived.reshape(ghosts_n, latent)
    fine_out, window, pre, node_pre, summed = call(
        functools.partial(forward_kernel, chunk),
        [((rows, latent), BF16), ((co + 2 * BAND, latent), F32), ((edges_n, latent), F32),
         ((rows, latent), F32), ((rows, latent), BF16)],
        [pltpu.VMEM((rows + ghosts_n, latent), BF16), pltpu.VMEM((fold_all, FOLDS * latent), BF16),
         pltpu.VMEM((fold_rows, FOLDS * latent), BF16), pltpu.VMEM((edges_n, FOLDS * latent), BF16)],
        (nodes, ghosts, edge_send, edge_recv, edge_total, pool_map, w_edge_in, w_edge_out, w_node_in, w_node_out))
    coarse_out, reach, g_ci, g_co = call(
        functools.partial(coarse_kernel, n_gy),
        [((co, latent), BF16), ((co + 2 * BAND, latent), BF16), ((latent, latent), F32), ((latent, latent), F32)],
        [pltpu.VMEM((2, BAND, latent), BF16)] * 4 + [dma((2, 2)), dma((2, 2))],
        (window, d_coarse, w_coarse_in, w_coarse_out), 1)
    d_owned, d_ghosts, partial = call(
        functools.partial(backward_kernel, chunk),
        [((rows, latent), F32), ((ghosts_n, latent), BF16), ((8 * latent, latent), F32)],
        [pltpu.VMEM((fold_rows, FOLDS * latent), BF16), pltpu.VMEM((edges_n, FOLDS * latent), BF16),
         pltpu.VMEM((edges_n, FOLDS * latent), BF16), pltpu.VMEM((rows + ghosts_n, latent), BF16),
         pltpu.VMEM((rows, latent), BF16), pltpu.VMEM((latent, latent), F32)],
        (nodes, ghosts, edge_recv, edge_total, edge_send, pool_map, w_edge_in, w_edge_out, w_node_in,
         w_node_out, pre, node_pre, summed, reach, d_fine, g_ci, g_co))
    share = 8 * latent // (n_gx * n_gy)
    parts = (n_gx, n_gy, share, latent)
    back, total = call(
        functools.partial(reduce_kernel, n_gx, n_gy),
        [((peers, slots, latent), BF16), (parts, BF16)],
        [pltpu.VMEM(parts, BF16), pltpu.VMEM((n_gx - 1,) + parts[1:], BF16), pltpu.VMEM(parts[1:], BF16),
         pltpu.VMEM((n_gy - 1,) + parts[2:], BF16), dma((peers,)), dma((peers,))]
        + [dma((n_gx - 1,))] * 2 + [dma((n_gy - 1,))] * 2 + [dma((n_gx - 1,))] * 2 + [dma((n_gy - 1,))] * 2,
        (d_ghosts.reshape(peers, slots, latent), partial.reshape(parts)), 2)
    scale = 1.0 / (rows * n_gx * n_gy) ** 0.5
    outs = call(
        functools.partial(final_kernel, scale),
        [((rows, latent), F32), ((2 * latent, latent), F32), ((latent, latent), F32), ((2 * latent, latent), F32),
         ((latent, latent), F32), ((latent, latent), F32), ((latent, latent), F32)],
        [pltpu.VMEM((ghosts_n, FOLDS * latent), BF16)],
        (d_owned, back, ghost_rows, ghost_count, total.reshape(8 * latent, latent)))
    return (fine_out, coarse_out) + tuple(outs)


def solution(mesh):
    split = P(("gx", "gy"), None)
    return jax.shard_map(
        functools.partial(body, mesh.shape["gx"], mesh.shape["gy"]),
        mesh=mesh,
        in_specs=(split, P(("gx", "gy"), None, None), split, split, split, P(("gx", "gy")), split)
        + (P(),) * 6
        + (split, split),
        out_specs=(split, split, split) + (P(),) * 6,
        check_vma=False,
    )
```
